32 devices in a mesh: seq: 8 (over z, x), mem: 4 (over y, core).
Axes of the slice: x: 2, y: 2, z: 4, core: 2. Of those that a mesh axis runs over, the one named last changes fastest.
Arguments:
- queries: bfloat16 [4096, 2048], P(('seq', 'mem')), may hold values from -6 to 6
- keys: bfloat16 [4096, 2048], P(('seq', 'mem')), may hold values from -0.52734375 to 0.52734375
- values: bfloat16 [4096, 2048], P(('seq', 'mem')), may hold values from -6 to 6
- gamma: bfloat16 [4096, 16], P(('seq', 'mem')), as said below
- rate: bfloat16 [4, 16], replicated, as said below
- route_ids: int32 [4096, 2], P(('seq', 'mem')), may hold values from 0 to 3, all different within a row; in each aligned block of 128 rows (0 to 127, 128 to 255, ...) at most 96 rows name the same one
- route_weights: float32 [4096, 2], P(('seq', 'mem')), may hold values from 0.2 to 1
- norm_gain: float32 [2048], replicated, may hold values from 0.25 to 1.75
Outputs:
- mixed_out: bfloat16 [4096, 2048], P(('seq', 'mem'))
The draws below stay inside these ranges and needn't reach their ends.
Inputs may be any that keep to these rules, and one draw needn't show every extreme that they name: `route_ids`: each token names two different memories. The tokens of one device name one memory at most 96 times; some memory is named exactly 96 times by some device's tokens. `gamma`: Positive; from 0.5 up to 6144. `rate`: Positive; from 0.04 * 4 / 4096 up to 0.06.
All inputs are finite; a program needn't handle non-finite values.
Results may differ from the reference program's by a relative error of at most 0.0052.
Values may be sent and summed in bfloat16 or wider, within the bound.
A program may use at most 128 MiB of HBM per device.

```python
import math
import jax
import jax.numpy as jnp
import numpy as np
from jax import lax

TOK_DEV = 128
HEADS = 16
HD = 128
BLOCK = 128
MEMORY_COUNT = 4
C = 96
SEQUENCE_TOKENS = 4096
SLOTS = 3072
N_SEQ = 8
N_MEM = 4


def draw_gamma(key, part):
    key_base = jax.random.fold_in(key, 11)
    key_position = jax.random.fold_in(key, 12)
    key_size = jax.random.fold_in(key, 13)
    baseline_rows = jnp.exp(jax.random.uniform(key_base, (SEQUENCE_TOKENS, HEADS), jnp.float32, math.log(0.5), math.log(2.0)))
    spike_positions = jax.random.randint(key_position, (2 * MEMORY_COUNT,), 0, SEQUENCE_TOKENS)
    spike_mask = jnp.zeros((SEQUENCE_TOKENS,), jnp.float32).at[spike_positions].set(1.0)
    spike_magnitude = 4.4 * SEQUENCE_TOKENS / MEMORY_COUNT * jax.random.uniform(key_size, (SEQUENCE_TOKENS, 1), jnp.float32, 1.0, 1.2)
    return jnp.where(spike_mask[:, None] > 0.5, spike_magnitude, baseline_rows).astype(jnp.bfloat16)


def draw_rate(key, part):
    lowest = 0.05 * MEMORY_COUNT / SEQUENCE_TOKENS
    share = 0.5
    slow_pick = jax.random.uniform(jax.random.fold_in(key, 21), (MEMORY_COUNT, HEADS), jnp.float32) < share
    slow_rates = lowest * jnp.exp(jax.random.uniform(jax.random.fold_in(key, 22), (MEMORY_COUNT, HEADS), jnp.float32, 0.0, math.log(2.0)))
    fast_rates = jnp.exp(jax.random.uniform(jax.random.fold_in(key, 23), (MEMORY_COUNT, HEADS), jnp.float32, math.log(0.01), math.log(0.05)))
    return jnp.where(slow_pick, slow_rates, fast_rates).astype(jnp.bfloat16)


def steps_of(stream_key, shape, shards, low, largest):
    loudness = 1.0
    for axis_at, parts in shards:
        heights = jax.random.uniform(jax.random.fold_in(jax.random.fold_in(stream_key, 6), axis_at), (parts,), jnp.float32, low / len(shards), largest / len(shards))
        loudness = loudness * jnp.repeat(jnp.exp(heights), shape[axis_at] // parts).reshape((-1,) + (1,) * (len(shape) - 1 - axis_at))
    return loudness


def deal_out(own_key, own, number, rows, amount, top, bound, slope):
    sequence = jax.random.permutation(own_key, amount)
    packed, usual = load_shares(amount, rows * top, bound, slope, True), load_shares(amount, rows * top, bound, slope, False)
    places = jnp.arange(amount)

    def named(lengths, rotation):
        used = int((lengths > 0).sum())
        fixed = max(1, used // 4)
        moved = fixed + (places - fixed + rotation * (used - fixed)) % max(1, amount - fixed)
        return jnp.zeros((amount,), jnp.int32).at[sequence[jnp.where(places < fixed, places, moved)]].set(jnp.asarray(lengths, jnp.int32))

    lengths = jnp.where(number % 4 == 0, named(packed, number // 4), named(usual, number - number // 4 - 1))
    mixed = jax.random.permutation(jax.random.fold_in(own, 3), amount)
    giver, taker = mixed[0:amount // 2 * 2:2], mixed[1:amount // 2 * 2:2]
    room = jnp.minimum(lengths[giver] - 1, bound - lengths[taker]) // 2
    room = jnp.where((giver == sequence[0]) | (taker == sequence[0]) | (lengths[taker] == 0), 0, jnp.maximum(room, 0))
    moved = jax.random.randint(jax.random.fold_in(own, 4), (amount // 2,), 0, 1 << 20) % (room + 1)
    lengths = lengths.at[giver].add(-moved).at[taker].add(moved)
    items = jnp.searchsorted(jnp.cumsum(lengths), jnp.arange(rows * top), side="right").astype(jnp.int32)
    table = items.reshape(top, rows).T
    table = table[jax.random.permutation(jax.random.fold_in(own, 1), rows)]
    rotation = jax.random.randint(jax.random.fold_in(own, 2), (rows, 1), 0, top)
    return jnp.take_along_axis(table, (jnp.arange(top)[None, :] + rotation) % top, axis=1)


def load_shares(amount, total, limit, skew, full):
    portions = [(1 << 20) // math.isqrt(rank ** skew) + 1 for rank in range(1, amount + 1)]
    largest = limit if full else min(limit, max(-(-total // amount), total * portions[0] // sum(portions)))
    least = 1 if total - largest >= amount - 1 else 0
    given, rest = [largest] + [least] * (amount - 1), total - largest - least * (amount - 1)
    while rest > 0:
        movable = [i for i in range(1, amount) if given[i] < largest] or [i for i in range(1, amount) if given[i] < limit]
        mass, budget = sum([portions[i] for i in movable]), rest
        for i in movable:
            addition = min(limit - given[i], max(1, budget * portions[i] // mass), rest)
            given[i] = given[i] + addition
            rest = rest - addition
    return np.array(given)


def centred(stream_key, dims, scale, most, split=(), kind=jnp.bfloat16):
    values = scale * jax.random.normal(stream_key, dims, jnp.float32)
    if split:
        values = values * steps_of(stream_key, dims, split, -0.22, 0.18)
    return jnp.clip(values, -most, most).astype(kind)


def setup_inputs(seed: int = 0) -> dict:
    key_list = jax.random.split(jax.random.key(seed), 9)
    queries = centred(key_list[0], (SEQUENCE_TOKENS, HEADS * HD), 1.0, 6.0, ((0, 32),))
    keys = centred(key_list[1], (SEQUENCE_TOKENS, HEADS * HD), 0.088, 0.52734375, ((0, 32),))
    values = centred(key_list[2], (SEQUENCE_TOKENS, HEADS * HD), 1.0, 6.0, ((0, 32),))
    gamma = draw_gamma(jax.random.fold_in(key_list[8], 71), 0)
    rate = draw_rate(jax.random.fold_in(key_list[8], 71), 0)
    route_ids_keys = jax.random.split(jax.random.fold_in(key_list[5], 1), SEQUENCE_TOKENS // TOK_DEV)
    route_ids_turns = jax.random.permutation(jax.random.fold_in(key_list[5], 3), SEQUENCE_TOKENS // TOK_DEV)
    route_ids = jax.vmap(lambda own, number: deal_out(jax.random.fold_in(key_list[5], 2), own, number, TOK_DEV, MEMORY_COUNT, 2, C, 2))(route_ids_keys, route_ids_turns).reshape((SEQUENCE_TOKENS, 2))
    route_weights = jnp.clip(0.2 + 0.8 * jax.random.uniform(key_list[6], (SEQUENCE_TOKENS, 2), jnp.float32) ** steps_of(key_list[6], (SEQUENCE_TOKENS, 2), ((0, 32),), -0.2, 0.2), 0.2, 1.0)
    norm_gain = jnp.clip(1.0 + 0.15 * jax.random.normal(key_list[7], (HEADS * HD,), jnp.float32), 0.25, 1.75)
    return dict(queries=queries, keys=keys, values=values, gamma=gamma, rate=rate, route_ids=route_ids, route_weights=route_weights, norm_gain=norm_gain)


epsilon = 1e-06

def reference(queries, keys, values, gamma, rate, route_ids, route_weights, norm_gain):
    feat_count = HEADS * HD
    block_count = SLOTS // BLOCK
    device_ids = (jnp.arange(SEQUENCE_TOKENS, dtype=jnp.int32) // TOK_DEV).astype(jnp.int32)
    causal = (jnp.arange(BLOCK)[:, None] >= jnp.arange(BLOCK)[None, :])[:, :, None]
    highest = lax.Precision.HIGHEST

    def memory_pass(totals, memory):
        route_hits = (route_ids == memory).astype(jnp.int32)
        route_rank = (jnp.cumsum(route_hits.reshape(N_SEQ * N_MEM, TOK_DEV * 2), axis=1).astype(jnp.int32).reshape(SEQUENCE_TOKENS, 2) - 1).astype(jnp.int32)
        token_rank = lax.optimization_barrier(jnp.sum(route_hits * route_rank, axis=1)).astype(jnp.int32)
        routed = lax.optimization_barrier(jnp.sum(route_hits, axis=1))
        slot_ids = jnp.where(routed > 0, device_ids * C + token_rank, SLOTS).astype(jnp.int32)
        query_slots = jnp.zeros((SLOTS, feat_count), jnp.bfloat16).at[slot_ids].set(queries, mode='drop')
        key_slots = jnp.zeros((SLOTS, feat_count), jnp.bfloat16).at[slot_ids].set(keys, mode='drop')
        value_slots = jnp.zeros((SLOTS, feat_count), jnp.bfloat16).at[slot_ids].set(values, mode='drop')
        gamma_slots = jnp.zeros((SLOTS, HEADS), jnp.bfloat16).at[slot_ids].set(gamma, mode='drop')
        rate_now = rate[memory].astype(jnp.float32)

        def block_step(state_now, inputs_now):
            query_rows, key_rows, value_rows, gamma_rows = inputs_now
            query32 = query_rows.astype(jnp.float32)
            key32 = key_rows.astype(jnp.float32)
            value32 = value_rows.astype(jnp.float32)
            levels = jnp.cumsum(-rate_now[None, :] * gamma_rows.astype(jnp.float32), axis=0)
            spread_log = levels[:, None, :] - levels[None, :, :]
            decays = jnp.exp(jnp.where(causal, spread_log, -1e+30))
            scores = jnp.einsum('thd,shd->tsh', query32, key32, precision=highest)
            weights = lax.optimization_barrier((decays * scores).astype(jnp.bfloat16)).astype(jnp.float32)
            intra_out = jnp.einsum('tsh,she->the', weights, value32, precision=highest)
            inter_out = jnp.einsum('thd,hde->the', query32 * jnp.exp(levels)[:, :, None], state_now, precision=highest)
            raw_out = intra_out + inter_out
            normed = raw_out * lax.rsqrt(lax.optimization_barrier(jnp.mean(raw_out * raw_out, axis=-1, keepdims=True)) + epsilon)
            last_level = levels[-1]
            keyed_rows = lax.optimization_barrier((key32 * jnp.exp(last_level[None, :] - levels)[:, :, None]).astype(jnp.bfloat16)).astype(jnp.float32)
            state_next = jnp.exp(last_level)[:, None, None] * state_now + jnp.einsum('shd,she->hde', keyed_rows, value32, precision=highest)
            return (state_next, normed.astype(jnp.bfloat16))
        start_state = jnp.zeros((HEADS, HD, HD), jnp.float32)
        block_inputs = (query_slots.reshape(block_count, BLOCK, HEADS, HD), key_slots.reshape(block_count, BLOCK, HEADS, HD), value_slots.reshape(block_count, BLOCK, HEADS, HD), gamma_slots.reshape(block_count, BLOCK, HEADS))
        _, block_outs = lax.scan(block_step, start_state, block_inputs)
        block_outs = block_outs.reshape(SLOTS, feat_count)
        picked = jnp.take(block_outs, jnp.minimum(slot_ids, SLOTS - 1), axis=0).astype(jnp.float32)
        weight = lax.optimization_barrier(jnp.sum(jnp.where(route_hits > 0, route_weights, jnp.float32(0.0)), axis=1))
        return (totals + weight[:, None] * picked, None)
    totals, _ = lax.scan(memory_pass, jnp.zeros((SEQUENCE_TOKENS, feat_count), jnp.float32), jnp.arange(N_MEM, dtype=jnp.int32))
    return (totals * norm_gain[None, :]).astype(jnp.bfloat16)
```

```python
import functools

import jax
import jax.numpy as jnp
from jax import lax
from jax.experimental import pallas as pl
from jax.experimental.pallas import tpu as pltpu
from jax.sharding import PartitionSpec as P

EPSILON = 1e-06
FAR = 1e30
F32 = jnp.float32
BF16 = jnp.bfloat16
MESH = pl.DeviceIdType.MESH

KEYS_AT = 6400
HEAD_STEP = 2860
QUERY_STEP = 1430
RELAY_AT = 9200
RELAY_STEP = 700
HOP = 2350
UPDATE_NS = 450
INTRA_NS = 250
FINISH_NS = 600


def dot(a, b, dims=((1,), (0,))):
    return lax.dot_general(a, b, (dims, ((), ())), preferred_element_type=F32)


def kernel(n, seqs, hl, mems, pair, q_ref, k_ref, v_ref, gamma_ref, rate_ref,
           ids_ref, wts_ref, gain_ref, out_ref,
           qbuf, kbuf, vbuf, gbuf, ibuf, wbuf, ratev, gainv, lrm, kew, adec, atot, apart, cols, wide, maskb,
           pbuf, xbuf, u32, ubf, upart, esend, erecv, sgrp, raw, outb,
           aux_s, aux_r, tok_s, tok_r, loc_s, a_s, a_r, u_s, u_r, e_s, e_r, o_s, o_r, own_s):
    me = lax.axis_index("mem")
    pos = lax.axis_index("seq")
    tok = qbuf.shape[2]
    hd = qbuf.shape[3]
    heads = gbuf.shape[1]
    inner = lax.rem(pos, pair)
    even = inner == 0
    mate = pos + 1 - 2 * inner
    first = pos < pair
    last = pos + pair >= seqs
    rank = lax.div(pos, pair)

    def twin(device):
        return device + 1 - 2 * lax.rem(device, 2)

    near = [twin(me)]
    away = []
    for step in range(1, n // 2):
        there = lax.rem(me + 2 * step, n)
        away += [there, twin(there)]
    peers = away + near

    def lanes(head):
        return pl.ds(pl.multiple_of(head * hd, hd), hd)

    def token_copy(t, h, dst, slot):
        src, buf = ((k_ref, kbuf), (v_ref, vbuf), (q_ref, qbuf))[t]
        return pltpu.make_async_remote_copy(
            src_ref=src.at[:, lanes(dst * hl + h)], dst_ref=buf.at[slot, h],
            send_sem=tok_s.at[t, h, dst], recv_sem=tok_r.at[t, h, slot],
            device_id={"mem": dst}, device_id_type=MESH)

    def own_token(t, h):
        src, buf = ((k_ref, kbuf), (v_ref, vbuf), (q_ref, qbuf))[t]
        return pltpu.make_async_copy(src.at[:, lanes(me * hl + h)], buf.at[me, h], tok_s.at[t, h, me])

    def aux_copy(t, dst, slot):
        src, buf = ((gamma_ref, gbuf), (ids_ref, ibuf), (wts_ref, wbuf))[t]
        return pltpu.make_async_remote_copy(
            src_ref=src, dst_ref=buf.at[slot], send_sem=aux_s.at[t, dst], recv_sem=aux_r.at[t, slot],
            device_id={"mem": dst}, device_id_type=MESH)

    def own_aux(t):
        src, buf = ((gamma_ref, gbuf), (ids_ref, ibuf), (wts_ref, wbuf))[t]
        return pltpu.make_async_copy(src, buf.at[me], aux_s.at[t, me])

    def local_copy(t):
        src, buf = ((rate_ref, ratev), (gain_ref, gainv))[t]
        return pltpu.make_async_copy(src, buf, loc_s.at[t])

    def a_copy():
        return pltpu.make_async_remote_copy(
            src_ref=atot, dst_ref=apart, send_sem=a_s, recv_sem=a_r,
            device_id={"seq": mate}, device_id_type=MESH)

    def u_copy(h, m):
        return pltpu.make_async_remote_copy(
            src_ref=ubf.at[h, m], dst_ref=upart.at[h, m], send_sem=u_s.at[h, m], recv_sem=u_r.at[h, m],
            device_id={"seq": mate}, device_id_type=MESH)

    def e_copy(h, m):
        return pltpu.make_async_remote_copy(
            src_ref=esend.at[h, m], dst_ref=erecv.at[h, m], send_sem=e_s.at[h, m], recv_sem=e_r.at[h, m],
            device_id={"seq": lax.rem(pos + pair, seqs)}, device_id_type=MESH)

    def out_copy(h, dst, slot):
        return pltpu.make_async_remote_copy(
            src_ref=outb.at[h, dst], dst_ref=out_ref.at[:, lanes(slot * hl + h)],
            send_sem=o_s.at[h, dst], recv_sem=o_r.at[h, slot],
            device_id={"mem": dst}, device_id_type=MESH)

    def own_out(h):
        return pltpu.make_async_copy(outb.at[h, me], out_ref.at[:, lanes(me * hl + h)], own_s.at[h])

    barrier = pltpu.get_barrier_semaphore()

    def greet(**where):
        pl.semaphore_signal(barrier, inc=1, device_id=where, device_id_type=MESH)

    for there in peers:
        greet(mem=there)
    greet(seq=mate)

    @pl.when(jnp.logical_not(first))
    def _():
        greet(seq=pos - pair)

    @pl.when(jnp.logical_not(last))
    def _():
        greet(seq=pos + pair)

    for t in range(3):
        own_aux(t).start()
    for t in range(2):
        local_copy(t).start()
    for h in range(hl):
        for t in range(3):
            own_token(t, h).start()

    pl.semaphore_wait(barrier, n + jnp.minimum(rank, 1) + jnp.minimum(seqs // pair - 1 - rank, 1))

    for there in peers:
        for t in range(3):
            aux_copy(t, there, me).start()
    for h in range(hl):
        for t in (0, 1):
            for there in peers:
                token_copy(t, h, there, me).start()
    for h in range(hl):
        for there in peers:
            token_copy(2, h, there, me).start()

    row_at = lax.broadcasted_iota(jnp.int32, (tok, tok), 0)
    col_at = lax.broadcasted_iota(jnp.int32, (tok, tok), 1)
    rows = hl * mems

    local_copy(0).wait()
    table = ratev[...].astype(F32)
    head_at = lax.broadcasted_iota(jnp.int32, table.shape, 1)
    rates = jnp.concatenate(
        [jnp.sum(jnp.where(head_at == me * hl + h, table, 0.0), axis=1, keepdims=True) for h in range(hl)], axis=0)
    upper = (row_at <= col_at).astype(BF16)
    chosen = me * hl + lax.div(lax.broadcasted_iota(jnp.int32, (rows, heads), 0), mems)
    pick = (lax.broadcasted_iota(jnp.int32, (rows, heads), 1) == chosen).astype(BF16)
    for t in range(3):
        own_aux(t).wait()
        for there in peers:
            aux_copy(t, there, there).wait_recv()

    total = jnp.zeros((rows, tok), F32)
    mem_at = lax.rem(lax.broadcasted_iota(jnp.int32, (rows, tok), 0), mems)
    for j in range(n):
        ids = ibuf[j]
        hit = [ids[r:r + 1, :] == mem_at for r in (0, 1)]
        here = jnp.logical_or(hit[0], hit[1])
        picked = jnp.where(here, dot(pick, gbuf[j]), 0.0)
        level = -rates * dot(picked.astype(BF16), upper)
        end = jnp.broadcast_to(level[:, tok - 1:tok], level.shape)
        lrm[j] = jnp.where(here, level, FAR)
        kew[j] = jnp.where(here, jnp.exp(end - level), 0.0)
        adec[j] = jnp.exp(end)
        for h in range(hl):
            part = slice(h * mems, (h + 1) * mems)
            own = level[part]
            ahead = own + total[part]
            levels = [jnp.sum(jnp.where(hit[r][part], own, 0.0), axis=0, keepdims=True) for r in (0, 1)]
            aheads = [jnp.sum(jnp.where(hit[r][part], ahead, 0.0), axis=0, keepdims=True) for r in (0, 1)]
            stack = levels + [jnp.exp(x) for x in levels] + [jnp.exp(x) for x in aheads]
            cols[j, h] = jnp.concatenate(stack + [jnp.zeros((2, tok), F32)], axis=0).T
        total = total + end
        side = jnp.concatenate([ids.astype(F32), wbuf[j], jnp.zeros((4, tok), F32)], axis=0).T
        for c in range(4):
            wide[j, c] = jnp.broadcast_to(side[:, c:c + 1], (tok, hd))
        for r in (0, 1):
            for m in range(mems):
                maskb[j, r, m] = (side[:, r:r + 1] == float(m)).astype(F32).astype(BF16) * jnp.ones((tok, hd), BF16)
    atot[...] = jnp.exp(total)
    a_copy().start()
    for h in range(hl):
        pbuf[h, 0] = jnp.zeros((mems * hd, hd), BF16)

    def update(h):
        for t in (0, 1):
            own_token(t, h).wait()
            for there in peers:
                token_copy(t, h, there, there).wait_recv()
        state = jnp.zeros((mems * hd, hd), F32)
        for j in range(n):
            turned = kbuf[j, h].astype(F32).T
            keyed = jnp.concatenate(
                [(turned * kew[j, pl.ds(h * mems + m, 1), :]).astype(BF16) for m in range(mems)], axis=0)
            fresh = dot(keyed, vbuf[j, h])
            if j > 0:
                pbuf[h, j] = state.astype(BF16)
                state = jnp.concatenate(
                    [adec[j, pl.ds(h * mems + m, 1), :] * state[m * hd:(m + 1) * hd] for m in range(mems)],
                    axis=0) + fresh
            else:
                state = fresh
        for m in range(mems):
            u32[h, m] = state[m * hd:(m + 1) * hd]
            ubf[h, m] = state[m * hd:(m + 1) * hd].astype(BF16)
            u_copy(h, m).start()

    causal = row_at >= col_at

    def intra(h, j):
        query, value = qbuf[j, h], vbuf[j, h]
        score = dot(query, kbuf[j, h], ((1,), (1,)))
        query32 = query.astype(F32)
        col = cols[j, h]
        levels = [lrm[j, pl.ds(h * mems + m, 1), :] for m in range(mems)]
        left = []
        for r in (0, 1):
            ident = wide[j, r]
            level = levels[0]
            for m in range(1, mems):
                level = jnp.where(ident == float(m), levels[m], level)
            decay = jnp.exp(jnp.where(causal, col[:, r:r + 1] - level, -FAR))
            near_query = (query32 * col[:, 2 + r:3 + r]).astype(BF16)
            far_query = (query32 * col[:, 4 + r:5 + r]).astype(BF16)
            left.append(jnp.concatenate(
                [(decay * score).astype(BF16)] + [near_query * maskb[j, r, m] for m in range(mems)], axis=1))
            for m in range(mems):
                xbuf[h, j, r * tok:(r + 1) * tok, m * hd:(m + 1) * hd] = far_query * maskb[j, r, m]
        raw[h, j] = dot(jnp.concatenate(left, axis=0), jnp.concatenate([value, pbuf[h, j]], axis=0))

    def relay(unit, carry):
        h = lax.div(unit, mems)
        m = lax.rem(unit, mems)

        @pl.when(unit == 0)
        def _():
            a_copy().wait_recv()

        mine, other = atot[pl.ds(unit, 1), :], apart[pl.ds(unit, 1), :]
        u_copy(h, m).wait_recv()

        @pl.when(first)
        def _():
            erecv[h, m] = jnp.zeros((hd, hd), BF16)

        @pl.when(jnp.logical_not(first))
        def _():
            e_copy(h, m).wait_recv()

        @pl.when(jnp.logical_not(last))
        def _():
            both = jnp.where(even, other, 1.0) * u32[h, m]
            both = both + jnp.where(even, 1.0, mine) * upart[h, m].astype(F32)
            esend[h, m] = (both + mine * other * erecv[h, m].astype(F32)).astype(BF16)
            e_copy(h, m).start()

        @pl.when(even)
        def _():
            sgrp[h, m] = erecv[h, m]

        @pl.when(jnp.logical_not(even))
        def _():
            sgrp[h, m] = (other * erecv[h, m].astype(F32) + upart[h, m].astype(F32)).astype(BF16)

        return carry

    def finish(h, j):
        gain = gainv[:, lanes(me * hl + h)]
        state = jnp.concatenate([sgrp[h, m] for m in range(mems)], axis=0)
        whole = raw[h, j] + dot(xbuf[h, j], state)
        mixed = jnp.zeros((tok, hd), F32)
        for r in (0, 1):
            part = whole[r * tok:(r + 1) * tok]
            scale = lax.rsqrt(jnp.mean(part * part, axis=-1, keepdims=True) + EPSILON)
            mixed = mixed + wide[j, 2 + r] * (part * scale).astype(BF16).astype(F32)
        outb[h, j] = (mixed * gain).astype(BF16)

    done = [0]

    def catch_up(now, low, high):
        upto = jnp.clip(lax.div(now - RELAY_AT - rank * HOP + 100 * RELAY_STEP, RELAY_STEP) - 99,
                        low * mems, high * mems)
        lax.fori_loop(done[0], upto, relay, 0)
        done[0] = upto

    for h in range(hl):
        update(h)
        now = KEYS_AT + h * HEAD_STEP + UPDATE_NS
        catch_up(now, 0, h)
        own_token(2, h).wait()
        token_copy(2, h, near[0], near[0]).wait_recv()
        for j in [me] + near:
            intra(h, j)
            now += INTRA_NS
            catch_up(now, 0, h + 1)
        if h + 1 < hl:
            catch_up(KEYS_AT + (h + 1) * HEAD_STEP, 0, h + 1)

    def finish_all(h):
        for there in peers:
            finish(h, there)
            out_copy(h, there, me).start()
        finish(h, me)
        own_out(h).start()

    local_copy(1).wait()
    queries_at = KEYS_AT + (hl - 1) * HEAD_STEP + QUERY_STEP
    for h in range(hl):
        catch_up(queries_at + h * QUERY_STEP, max(h - 1, 0), hl)
        for i, there in enumerate(away):
            token_copy(2, h, there, there).wait_recv()
            intra(h, there)
            catch_up(queries_at + h * QUERY_STEP + (i + 1) * INTRA_NS, max(h - 1, 0), hl)
        if h == 1:
            catch_up(queries_at + h * QUERY_STEP + 2 * INTRA_NS, 1, hl)
            finish_all(0)
    for h in range(1 if hl > 1 else 0, hl):
        catch_up(queries_at + hl * QUERY_STEP + h * FINISH_NS, h + 1, hl)
        finish_all(h)

    for h in range(hl):
        own_out(h).wait()
    for there in peers:
        for t in range(3):
            aux_copy(t, there, me).wait_send()
        for h in range(hl):
            for t in range(3):
                token_copy(t, h, there, me).wait_send()
            out_copy(h, there, me).wait_send()
            out_copy(h, there, there).wait_recv()
    a_copy().wait_send()
    for h in range(hl):
        for m in range(mems):
            u_copy(h, m).wait_send()

            @pl.when(jnp.logical_not(last))
            def _():
                e_copy(h, m).wait_send()


def body(n, seqs, queries, keys, values, gamma, rate, route_ids, route_weights, norm_gain):
    tok, feats = queries.shape
    heads = gamma.shape[1]
    mems = rate.shape[0]
    hd = feats // heads
    hl = heads // n
    pair = 2
    vm = pltpu.VMEM
    dma = pltpu.SemaphoreType.DMA
    rows = hl * mems
    scratch = [
        vm((n, hl, tok, hd), BF16), vm((n, hl, tok, hd), BF16), vm((n, hl, tok, hd), BF16),
        vm((n, heads, tok), BF16), vm((n, 2, tok), jnp.int32), vm((n, 2, tok), F32),
        vm(rate.shape, BF16), vm((1, feats), F32),
        vm((n, rows, tok), F32), vm((n, rows, tok), F32), vm((n, rows, tok), F32),
        vm((rows, tok), F32), vm((rows, tok), F32),
        vm((n, hl, tok, 8), F32), vm((n, 4, tok, hd), F32), vm((n, 2, mems, tok, hd), BF16),
        vm((hl, n, mems * hd, hd), BF16), vm((hl, n, 2 * tok, mems * hd), BF16),
        vm((hl, mems, hd, hd), F32), vm((hl, mems, hd, hd), BF16), vm((hl, mems, hd, hd), BF16),
        vm((hl, mems, hd, hd), BF16), vm((hl, mems, hd, hd), BF16), vm((hl, mems, hd, hd), BF16),
        vm((hl, n, 2 * tok, hd), F32),
        vm((hl, n, tok, hd), BF16),
        dma((3, n)), dma((3, n)), dma((3, hl, n)), dma((3, hl, n)), dma((2,)), dma, dma,
        dma((hl, mems)), dma((hl, mems)), dma((hl, mems)), dma((hl, mems)), dma((hl, n)), dma((hl, n)), dma((hl,)),
    ]
    spec = pl.BlockSpec(memory_space=pl.ANY)
    return pl.pallas_call(
        functools.partial(kernel, n, seqs, hl, mems, pair),
        out_shape=jax.ShapeDtypeStruct((tok, feats), BF16),
        in_specs=[spec] * 8,
        out_specs=spec,
        scratch_shapes=scratch,
        compiler_params=pltpu.CompilerParams(
            collective_id=0, has_side_effects=True, vmem_limit_bytes=60 * 1024 * 1024),
    )(queries, keys, values, gamma.T, rate, route_ids.T, route_weights.T, norm_gain.reshape(1, feats))


def solution(mesh):
    rows = P(("seq", "mem"), None)
    in_specs = (rows, rows, rows, rows, P(), rows, rows, P())
    run = functools.partial(body, mesh.shape["mem"], mesh.shape["seq"])
    return jax.shard_map(run, mesh=mesh, in_specs=in_specs, out_specs=rows, check_vma=False)
```

```python
import functools
import math

import jax
import jax.numpy as jnp
from jax import lax
from jax.experimental import pallas as pl
from jax.experimental.pallas import tpu as pltpu
from jax.sharding import PartitionSpec as P

EPSILON = 1e-06
FAR = 1e30
F32 = jnp.float32
BF16 = jnp.bfloat16
MESH = pl.DeviceIdType.MESH

KEYS_AT = 8400
HEAD_STEP = 2860
QUERY_STEP = 1430
EARLY_AT = 8850
LATE_AT = 12000
PIECE_STEP = 700
HOP = 1900
UPDATE_NS = 450
INTRA_NS = 360
FINISH_NS = 600


def dot(a, b, dims=((1,), (0,))):
    return lax.dot_general(a, b, (dims, ((), ())), preferred_element_type=F32)


def kernel(n, seqs, hl, mems, pair, q_ref, k_ref, v_ref, gamma_ref, rate_ref,
           ids_ref, wts_ref, gain_ref, out_ref,
           qbuf, kbuf, vbuf, gbuf, ibuf, wbuf, ratev, gainv, lrm, kew, adec, atot, apart, cols, wide, maskb,
           pbuf, xbuf, u32, ubf, upart, esend, erecv, sgrp, raw, outb,
           aux_s, aux_r, tok_s, tok_r, loc_s, a_s, a_r, u_s, u_r, e_s, e_r, o_s, o_r, own_s):
    me = lax.axis_index("mem")
    pos = lax.axis_index("seq")
    tok = qbuf.shape[2]
    hd = qbuf.shape[3]
    heads = gbuf.shape[1]
    inner = lax.rem(pos, pair)
    even = inner == 0
    mate = pos + 1 - 2 * inner
    first = pos < pair
    last = pos + pair >= seqs
    rank = lax.div(pos, pair)

    def twin(device):
        return device + 1 - 2 * lax.rem(device, 2)

    near = [twin(me)]
    away = []
    for step in range(1, n // 2):
        there = lax.rem(me + 2 * step, n)
        away += [there, twin(there)]
    peers = away + near
    turned_later = mems // 2
    direct = mems - turned_later

    def lanes(head):
        return pl.ds(pl.multiple_of(head * hd, hd), hd)

    def token_copy(t, h, dst, slot):
        src, buf = ((k_ref, kbuf), (v_ref, vbuf), (q_ref, qbuf))[t]
        return pltpu.make_async_remote_copy(
            src_ref=src.at[:, lanes(dst * hl + h)], dst_ref=buf.at[slot, h],
            send_sem=tok_s.at[t, h, dst], recv_sem=tok_r.at[t, h, slot],
            device_id={"mem": dst}, device_id_type=MESH)

    def own_token(t, h):
        src, buf = ((k_ref, kbuf), (v_ref, vbuf), (q_ref, qbuf))[t]
        return pltpu.make_async_copy(src.at[:, lanes(me * hl + h)], buf.at[me, h], tok_s.at[t, h, me])

    def aux_copy(t, dst, slot):
        src, buf = ((gamma_ref, gbuf), (ids_ref, ibuf), (wts_ref, wbuf))[t]
        return pltpu.make_async_remote_copy(
            src_ref=src, dst_ref=buf.at[slot], send_sem=aux_s.at[t, dst], recv_sem=aux_r.at[t, slot],
            device_id={"mem": dst}, device_id_type=MESH)

    def own_aux(t):
        src, buf = ((gamma_ref, gbuf), (ids_ref, ibuf), (wts_ref, wbuf))[t]
        return pltpu.make_async_copy(src, buf.at[me], aux_s.at[t, me])

    def local_copy(t):
        src, buf = ((rate_ref, ratev), (gain_ref, gainv))[t]
        return pltpu.make_async_copy(src, buf, loc_s.at[t])

    def a_copy():
        return pltpu.make_async_remote_copy(
            src_ref=atot, dst_ref=apart, send_sem=a_s, recv_sem=a_r,
            device_id={"seq": mate}, device_id_type=MESH)

    def u_copy(h, m):
        return pltpu.make_async_remote_copy(
            src_ref=ubf.at[h, m], dst_ref=upart.at[h, m], send_sem=u_s.at[h, m], recv_sem=u_r.at[h, m],
            device_id={"seq": mate}, device_id_type=MESH)

    def e_copy(h, m):
        return pltpu.make_async_remote_copy(
            src_ref=esend.at[h, m], dst_ref=erecv.at[h, m], send_sem=e_s.at[h, m], recv_sem=e_r.at[h, m],
            device_id={"seq": lax.rem(pos + pair, seqs)}, device_id_type=MESH)

    def out_copy(h, dst, slot):
        return pltpu.make_async_remote_copy(
            src_ref=outb.at[h, dst], dst_ref=out_ref.at[:, lanes(slot * hl + h)],
            send_sem=o_s.at[h, dst], recv_sem=o_r.at[h, slot],
            device_id={"mem": dst}, device_id_type=MESH)

    def own_out(h):
        return pltpu.make_async_copy(outb.at[h, me], out_ref.at[:, lanes(me * hl + h)], own_s.at[h])

    barrier = pltpu.get_barrier_semaphore()

    def greet(**where):
        pl.semaphore_signal(barrier, inc=1, device_id=where, device_id_type=MESH)

    for there in peers:
        greet(mem=there)
    greet(seq=mate)

    @pl.when(jnp.logical_not(first))
    def _():
        greet(seq=pos - pair)

    @pl.when(jnp.logical_not(last))
    def _():
        greet(seq=pos + pair)

    for t in range(3):
        own_aux(t).start()
    for t in range(2):
        local_copy(t).start()
    for h in range(hl):
        for t in range(3):
            own_token(t, h).start()

    pl.semaphore_wait(barrier, n + jnp.minimum(rank, 1) + jnp.minimum(seqs // pair - 1 - rank, 1))

    for there in peers:
        for t in range(3):
            aux_copy(t, there, me).start()
    for h in range(hl):
        for t in (0, 1):
            for there in peers:
                token_copy(t, h, there, me).start()
    for h in range(hl):
        for there in peers:
            token_copy(2, h, there, me).start()

    row_at = lax.broadcasted_iota(jnp.int32, (tok, tok), 0)
    col_at = lax.broadcasted_iota(jnp.int32, (tok, tok), 1)
    rows = hl * mems

    local_copy(0).wait()
    table = ratev[...].astype(F32)
    head_at = lax.broadcasted_iota(jnp.int32, table.shape, 1)
    rates = jnp.concatenate(
        [jnp.sum(jnp.where(head_at == me * hl + h, table, 0.0), axis=1, keepdims=True) for h in range(hl)], axis=0)
    upper = (row_at <= col_at).astype(BF16)
    chosen = me * hl + lax.div(lax.broadcasted_iota(jnp.int32, (rows, heads), 0), mems)
    pick = (lax.broadcasted_iota(jnp.int32, (rows, heads), 1) == chosen).astype(BF16)
    for t in range(3):
        own_aux(t).wait()
        for there in peers:
            aux_copy(t, there, there).wait_recv()

    total = jnp.zeros((rows, tok), F32)
    mem_at = lax.rem(lax.broadcasted_iota(jnp.int32, (rows, tok), 0), mems)
    for j in range(n):
        ids = ibuf[j]
        hit = [ids[r:r + 1, :] == mem_at for r in (0, 1)]
        here = jnp.logical_or(hit[0], hit[1])
        picked = jnp.where(here, dot(pick, gbuf[j]), 0.0)
        level = -rates * dot(picked.astype(BF16), upper)
        end = jnp.broadcast_to(level[:, tok - 1:tok], level.shape)
        lrm[j] = jnp.where(here, level, FAR)
        kew[j] = jnp.where(here, jnp.exp(end - level), 0.0)
        adec[j] = jnp.exp(end)
        for h in range(hl):
            part = slice(h * mems, (h + 1) * mems)
            own = level[part]
            ahead = own + total[part]
            levels = [jnp.sum(jnp.where(hit[r][part], own, 0.0), axis=0, keepdims=True) for r in (0, 1)]
            aheads = [jnp.sum(jnp.where(hit[r][part], ahead, 0.0), axis=0, keepdims=True) for r in (0, 1)]
            stack = levels + [jnp.exp(x) for x in levels] + [jnp.exp(x) for x in aheads]
            cols[j, h] = jnp.concatenate(stack + [jnp.zeros((2, tok), F32)], axis=0).T
        total = total + end
        side = jnp.concatenate([ids.astype(F32), wbuf[j], jnp.zeros((4, tok), F32)], axis=0).T
        for c in range(4):
            wide[j, c] = jnp.broadcast_to(side[:, c:c + 1], (tok, hd))
        for r in (0, 1):
            for m in range(mems):
                maskb[j, r, m] = (side[:, r:r + 1] == float(m)).astype(F32).astype(BF16) * jnp.ones((tok, hd), BF16)
    atot[...] = jnp.exp(total)
    a_copy().start()
    for h in range(hl):
        pbuf[h, 0] = jnp.zeros((mems * hd, hd), BF16)

    def update(h):
        for t in (0, 1):
            own_token(t, h).wait()
            for there in peers:
                token_copy(t, h, there, there).wait_recv()
        state = jnp.zeros((mems * hd, hd), F32)
        for j in range(n):
            turned = kbuf[j, h].astype(F32).T
            keyed = jnp.concatenate(
                [(turned * kew[j, pl.ds(h * mems + m, 1), :]).astype(BF16) for m in range(mems)], axis=0)
            fresh = dot(keyed, vbuf[j, h])
            if j > 0:
                pbuf[h, j] = state.astype(BF16)
                state = jnp.concatenate(
                    [adec[j, pl.ds(h * mems + m, 1), :] * state[m * hd:(m + 1) * hd] for m in range(mems)],
                    axis=0) + fresh
            else:
                state = fresh
        for m in range(mems):
            u32[h, m] = state[m * hd:(m + 1) * hd]
            if m < direct:
                ubf[h, m] = state[m * hd:(m + 1) * hd].astype(BF16)
                u_copy(h, m).start()

    causal = row_at >= col_at

    def intra(h, j):
        query, value = qbuf[j, h], vbuf[j, h]
        score = dot(query, kbuf[j, h], ((1,), (1,)))
        query32 = query.astype(F32)
        col = cols[j, h]
        levels = [lrm[j, pl.ds(h * mems + m, 1), :] for m in range(mems)]
        left = []
        for r in (0, 1):
            ident = wide[j, r]
            level = levels[0]
            for m in range(1, mems):
                level = jnp.where(ident == float(m), levels[m], level)
            decay = jnp.exp(jnp.where(causal, col[:, r:r + 1] - level, -FAR))
            near_query = (query32 * col[:, 2 + r:3 + r]).astype(BF16)
            far_query = (query32 * col[:, 4 + r:5 + r]).astype(BF16)
            left.append(jnp.concatenate(
                [(decay * score).astype(BF16)] + [near_query * maskb[j, r, m] for m in range(mems)], axis=1))
            for m in range(mems):
                xbuf[h, j, r * tok:(r + 1) * tok, m * hd:(m + 1) * hd] = far_query * maskb[j, r, m]
        raw[h, j] = dot(jnp.concatenate(left, axis=0), jnp.concatenate([value, pbuf[h, j]], axis=0))

    def receive(h, m):
        @pl.when(first)
        def _():
            erecv[h, m] = jnp.zeros((hd, hd), BF16)

        @pl.when(jnp.logical_not(first))
        def _():
            e_copy(h, m).wait_recv()

    def relay_early(unit, carry):
        h = lax.div(unit, turned_later)
        m = direct + lax.rem(unit, turned_later)
        mine, other = atot[pl.ds(h * mems + m, 1), :], apart[pl.ds(h * mems + m, 1), :]
        receive(h, m)
        before = erecv[h, m].astype(F32)
        fresh = u32[h, m]

        @pl.when(jnp.logical_not(last))
        def _():
            esend[h, m] = (jnp.where(even, other, 1.0) * fresh + mine * other * before).astype(BF16)
            e_copy(h, m).start()

        ubf[h, m] = jnp.where(even, mine * before + fresh, before).astype(BF16)
        u_copy(h, m).start()
        return carry

    def relay_late(unit, carry):
        h = lax.div(unit, mems)
        m = lax.rem(unit, mems)
        mine, other = atot[pl.ds(unit, 1), :], apart[pl.ds(unit, 1), :]
        u_copy(h, m).wait_recv()

        @pl.when(m < direct)
        def _():
            receive(h, m)

            @pl.when(jnp.logical_not(last))
            def _():
                both = jnp.where(even, other, 1.0) * u32[h, m]
                both = both + jnp.where(even, 1.0, mine) * upart[h, m].astype(F32)
                esend[h, m] = (both + mine * other * erecv[h, m].astype(F32)).astype(BF16)
                e_copy(h, m).start()

            @pl.when(even)
            def _():
                sgrp[h, m] = erecv[h, m]

            @pl.when(jnp.logical_not(even))
            def _():
                sgrp[h, m] = (other * erecv[h, m].astype(F32) + upart[h, m].astype(F32)).astype(BF16)

        @pl.when(m >= direct)
        def _():
            sgrp[h, m] = (jnp.where(even, 1.0, other) * erecv[h, m].astype(F32)
                          + upart[h, m].astype(F32)).astype(BF16)

        return carry

    def finish(h, j):
        gain = gainv[:, lanes(me * hl + h)]
        state = jnp.concatenate([sgrp[h, m] for m in range(mems)], axis=0)
        whole = raw[h, j] + dot(xbuf[h, j], state)
        mixed = jnp.zeros((tok, hd), F32)
        for r in (0, 1):
            part = whole[r * tok:(r + 1) * tok]
            scale = lax.rsqrt(jnp.mean(part * part, axis=-1, keepdims=True) + EPSILON)
            mixed = mixed + wide[j, 2 + r] * (part * scale).astype(BF16).astype(F32)
        outb[h, j] = (mixed * gain).astype(BF16)

    done = [0, 0]

    def catch_up(now, low, high):
        for stage, per, start in ((0, turned_later, EARLY_AT), (1, mems, LATE_AT)):
            since = now - start - rank * HOP + (64 + seqs) * HEAD_STEP
            whole = lax.div(since, HEAD_STEP)
            some = jnp.minimum(lax.div(since - whole * HEAD_STEP, PIECE_STEP) + 1, per)
            upto = jnp.clip((whole - 64 - seqs) * per + some, low * per, high * per)
            upto = jnp.maximum(upto, done[stage])
            lax.fori_loop(done[stage], upto, (relay_early, relay_late)[stage], 0)
            done[stage] = upto

    for h in range(hl):
        update(h)
        if h == 0:
            a_copy().wait_recv()
        now = KEYS_AT + h * HEAD_STEP + UPDATE_NS
        catch_up(now, 0, h + 1)
        own_token(2, h).wait()
        token_copy(2, h, near[0], near[0]).wait_recv()
        for j in [me] + near:
            intra(h, j)
            now += INTRA_NS
            catch_up(now, 0, h + 1)
        if h + 1 < hl:
            catch_up(KEYS_AT + (h + 1) * HEAD_STEP, 0, h + 1)

    def finish_all(h):
        for there in peers:
            finish(h, there)
            out_copy(h, there, me).start()
        finish(h, me)
        own_out(h).start()

    local_copy(1).wait()
    queries_at = KEYS_AT + (hl - 1) * HEAD_STEP + QUERY_STEP
    for h in range(hl):
        catch_up(queries_at + h * QUERY_STEP, max(h - 1, 0), hl)
        for i, there in enumerate(away):
            token_copy(2, h, there, there).wait_recv()
            intra(h, there)
            catch_up(queries_at + h * QUERY_STEP + (i + 1) * INTRA_NS, max(h - 1, 0), hl)
        if h == 1:
            catch_up(queries_at + h * QUERY_STEP + 2 * INTRA_NS, 1, hl)
            finish_all(0)
    for h in range(1 if hl > 1 else 0, hl):
        catch_up(queries_at + hl * QUERY_STEP + h * FINISH_NS, h + 1, hl)
        finish_all(h)

    for h in range(hl):
        own_out(h).wait()
    for there in peers:
        for t in range(3):
            aux_copy(t, there, me).wait_send()
        for h in range(hl):
            for t in range(3):
                token_copy(t, h, there, me).wait_send()
            out_copy(h, there, me).wait_send()
            out_copy(h, there, there).wait_recv()
    a_copy().wait_send()
    for h in range(hl):
        for m in range(mems):
            u_copy(h, m).wait_send()

            @pl.when(jnp.logical_not(last))
            def _():
                e_copy(h, m).wait_send()


def body(n, seqs, queries, keys, values, gamma, rate, route_ids, route_weights, norm_gain):
    tok, feats = queries.shape
    heads = gamma.shape[1]
    mems = rate.shape[0]
    hd = feats // heads
    hl = heads // n
    pair = 2
    vm = pltpu.VMEM
    dma = pltpu.SemaphoreType.DMA
    rows = hl * mems
    buffers = [
        vm((n, hl, tok, hd), BF16), vm((n, hl, tok, hd), BF16), vm((n, hl, tok, hd), BF16),
        vm((n, heads, tok), BF16), vm((n, 2, tok), jnp.int32), vm((n, 2, tok), F32),
        vm(rate.shape, BF16), vm((1, feats), F32),
        vm((n, rows, tok), F32), vm((n, rows, tok), F32), vm((n, rows, tok), F32),
        vm((rows, tok), F32), vm((rows, tok), F32),
        vm((n, hl, tok, 8), F32), vm((n, 4, tok, hd), F32), vm((n, 2, mems, tok, hd), BF16),
        vm((hl, n, mems * hd, hd), BF16), vm((hl, n, 2 * tok, mems * hd), BF16),
        vm((hl, mems, hd, hd), F32), vm((hl, mems, hd, hd), BF16), vm((hl, mems, hd, hd), BF16),
        vm((hl, mems, hd, hd), BF16), vm((hl, mems, hd, hd), BF16), vm((hl, mems, hd, hd), BF16),
        vm((hl, n, 2 * tok, hd), F32),
        vm((hl, n, tok, hd), BF16),
    ]
    scratch = buffers + [
        dma((3, n)), dma((3, n)), dma((3, hl, n)), dma((3, hl, n)), dma((2,)), dma, dma,
        dma((hl, mems)), dma((hl, mems)), dma((hl, mems)), dma((hl, mems)), dma((hl, n)), dma((hl, n)), dma((hl,)),
    ]
    held = sum(math.prod(x.shape) * jnp.dtype(x.dtype).itemsize for x in buffers)
    grant = min(held + held // 8 + (12 << 20), 60 << 20)
    spec = pl.BlockSpec(memory_space=pl.ANY)
    return pl.pallas_call(
        functools.partial(kernel, n, seqs, hl, mems, pair),
        out_shape=jax.ShapeDtypeStruct((tok, feats), BF16),
        in_specs=[spec] * 8,
        out_specs=spec,
        scratch_shapes=scratch,
        compiler_params=pltpu.CompilerParams(
            collective_id=0, has_side_effects=True, vmem_limit_bytes=grant),
    )(*[pltpu.with_memory_space_constraint(x, pltpu.HBM) for x in (queries, keys, values, gamma.T, rate, route_ids.T, route_weights.T, norm_gain.reshape(1, feats))])


def solution(mesh):
    rows = P(("seq", "mem"), None)
    in_specs = (rows, rows, rows, rows, P(), rows, rows, P())
    run = functools.partial(body, mesh.shape["mem"], mesh.shape["seq"])
    return jax.shard_map(run, mesh=mesh, in_specs=in_specs, out_specs=rows, check_vma=False)
```

```python
import functools
import math

import jax
import jax.numpy as jnp
from jax import lax
from jax.experimental import pallas as pl
from jax.experimental.pallas import tpu as pltpu
from jax.sharding import PartitionSpec as P

EPSILON = 1e-06
FAR = 1e30
F32 = jnp.float32
BF16 = jnp.bfloat16
MESH = pl.DeviceIdType.MESH

KEYS_AT = 8400
HEAD_STEP = 2860
QUERY_STEP = 1430
EARLY_AT = 8850
LATE_AT = 11700
PIECE_STEP = 700
HOP = 1900
UPDATE_NS = 450
INTRA_NS = 360
FINISH_NS = 600


def dot(a, b, dims=((1,), (0,))):
    return lax.dot_general(a, b, (dims, ((), ())), preferred_element_type=F32)


def kernel(n, seqs, hl, mems, pair, q_ref, k_ref, v_ref, gamma_ref, rate_ref,
           ids_ref, wts_ref, gain_ref, out_ref,
           qbuf, kbuf, vbuf, gbuf, ibuf, wbuf, ratev, gainv, lrm, kew, adec, atot, apart, cols, wide, maskb,
           pbuf, xbuf, u32, ubf, upart, esend, erecv, sgrp, raw, outb,
           aux_s, aux_r, tok_s, tok_r, loc_s, a_s, a_r, u_s, u_r, e_s, e_r, o_s, o_r, own_s):
    me = lax.axis_index("mem")
    pos = lax.axis_index("seq")
    tok = qbuf.shape[2]
    hd = qbuf.shape[3]
    heads = gbuf.shape[1]
    inner = lax.rem(pos, pair)
    even = inner == 0
    mate = pos + 1 - 2 * inner
    first = pos < pair
    last = pos + pair >= seqs
    rank = lax.div(pos, pair)

    def twin(device):
        return device + 1 - 2 * lax.rem(device, 2)

    near = [twin(me)]
    away = []
    for step in range(1, n // 2):
        there = lax.rem(me + 2 * step, n)
        away += [there, twin(there)]
    peers = away + near
    turned_later = mems // 2
    direct = mems - turned_later

    def lanes(head):
        return pl.ds(pl.multiple_of(head * hd, hd), hd)

    def token_copy(t, h, dst, slot):
        src, buf = ((k_ref, kbuf), (v_ref, vbuf), (q_ref, qbuf))[t]
        return pltpu.make_async_remote_copy(
            src_ref=src.at[:, lanes(dst * hl + h)], dst_ref=buf.at[slot, h],
            send_sem=tok_s.at[t, h, dst], recv_sem=tok_r.at[t, h, slot],
            device_id={"mem": dst}, device_id_type=MESH)

    def own_token(t, h):
        src, buf = ((k_ref, kbuf), (v_ref, vbuf), (q_ref, qbuf))[t]
        return pltpu.make_async_copy(src.at[:, lanes(me * hl + h)], buf.at[me, h], tok_s.at[t, h, me])

    def aux_copy(t, dst, slot):
        src, buf = ((gamma_ref, gbuf), (ids_ref, ibuf), (wts_ref, wbuf))[t]
        return pltpu.make_async_remote_copy(
            src_ref=src, dst_ref=buf.at[slot], send_sem=aux_s.at[t, dst], recv_sem=aux_r.at[t, slot],
            device_id={"mem": dst}, device_id_type=MESH)

    def own_aux(t):
        src, buf = ((gamma_ref, gbuf), (ids_ref, ibuf), (wts_ref, wbuf))[t]
        return pltpu.make_async_copy(src, buf.at[me], aux_s.at[t, me])

    def local_copy(t):
        src, buf = ((rate_ref, ratev), (gain_ref, gainv))[t]
        return pltpu.make_async_copy(src, buf, loc_s.at[t])

    def a_copy():
        return pltpu.make_async_remote_copy(
            src_ref=atot, dst_ref=apart, send_sem=a_s, recv_sem=a_r,
            device_id={"seq": mate}, device_id_type=MESH)

    def u_copy(h, m):
        return pltpu.make_async_remote_copy(
            src_ref=ubf.at[h, m], dst_ref=upart.at[h, m], send_sem=u_s.at[h, m], recv_sem=u_r.at[h, m],
            device_id={"seq": mate}, device_id_type=MESH)

    def e_copy(h, m):
        return pltpu.make_async_remote_copy(
            src_ref=esend.at[h, m], dst_ref=erecv.at[h, m], send_sem=e_s.at[h, m], recv_sem=e_r.at[h, m],
            device_id={"seq": lax.rem(pos + pair, seqs)}, device_id_type=MESH)

    def out_copy(h, dst, slot):
        return pltpu.make_async_remote_copy(
            src_ref=outb.at[h, dst], dst_ref=out_ref.at[:, lanes(slot * hl + h)],
            send_sem=o_s.at[h, dst], recv_sem=o_r.at[h, slot],
            device_id={"mem": dst}, device_id_type=MESH)

    def own_out(h):
        return pltpu.make_async_copy(outb.at[h, me], out_ref.at[:, lanes(me * hl + h)], own_s.at[h])

    barrier = pltpu.get_barrier_semaphore()

    def greet(**where):
        pl.semaphore_signal(barrier, inc=1, device_id=where, device_id_type=MESH)

    for there in peers:
        greet(mem=there)
    greet(seq=mate)

    @pl.when(jnp.logical_not(first))
    def _():
        greet(seq=pos - pair)

    @pl.when(jnp.logical_not(last))
    def _():
        greet(seq=pos + pair)

    for t in range(3):
        own_aux(t).start()
    for t in range(2):
        local_copy(t).start()
    for h in range(hl):
        for t in range(3):
            own_token(t, h).start()

    pl.semaphore_wait(barrier, n + jnp.minimum(rank, 1) + jnp.minimum(seqs // pair - 1 - rank, 1))

    for there in peers:
        for t in range(3):
            aux_copy(t, there, me).start()
    for h in range(hl):
        for t in (0, 1):
            for there in peers:
                token_copy(t, h, there, me).start()
    for h in range(hl):
        for there in peers:
            token_copy(2, h, there, me).start()

    row_at = lax.broadcasted_iota(jnp.int32, (tok, tok), 0)
    col_at = lax.broadcasted_iota(jnp.int32, (tok, tok), 1)
    rows = hl * mems

    local_copy(0).wait()
    table = ratev[...].astype(F32)
    head_at = lax.broadcasted_iota(jnp.int32, table.shape, 1)
    rates = jnp.concatenate(
        [jnp.sum(jnp.where(head_at == me * hl + h, table, 0.0), axis=1, keepdims=True) for h in range(hl)], axis=0)
    upper = (row_at <= col_at).astype(BF16)
    chosen = me * hl + lax.div(lax.broadcasted_iota(jnp.int32, (rows, heads), 0), mems)
    pick = (lax.broadcasted_iota(jnp.int32, (rows, heads), 1) == chosen).astype(BF16)
    for t in range(3):
        own_aux(t).wait()
        for there in peers:
            aux_copy(t, there, there).wait_recv()

    total = jnp.zeros((rows, tok), F32)
    mem_at = lax.rem(lax.broadcasted_iota(jnp.int32, (rows, tok), 0), mems)
    for j in range(n):
        ids = ibuf[j]
        hit = [ids[r:r + 1, :] == mem_at for r in (0, 1)]
        here = jnp.logical_or(hit[0], hit[1])
        picked = jnp.where(here, dot(pick, gbuf[j]), 0.0)
        level = -rates * dot(picked.astype(BF16), upper)
        end = jnp.broadcast_to(level[:, tok - 1:tok], level.shape)
        lrm[j] = jnp.where(here, level, FAR)
        kew[j] = jnp.where(here, jnp.exp(end - level), 0.0)
        adec[j] = jnp.exp(end)
        for h in range(hl):
            part = slice(h * mems, (h + 1) * mems)
            own = level[part]
            ahead = own + total[part]
            levels = [jnp.sum(jnp.where(hit[r][part], own, 0.0), axis=0, keepdims=True) for r in (0, 1)]
            aheads = [jnp.sum(jnp.where(hit[r][part], ahead, 0.0), axis=0, keepdims=True) for r in (0, 1)]
            stack = levels + [jnp.exp(x) for x in levels] + [jnp.exp(x) for x in aheads]
            cols[j, h] = jnp.concatenate(stack + [jnp.zeros((2, tok), F32)], axis=0).T
        total = total + end
        side = jnp.concatenate([ids.astype(F32), wbuf[j], jnp.zeros((4, tok), F32)], axis=0).T
        for c in range(4):
            wide[j, c] = jnp.broadcast_to(side[:, c:c + 1], (tok, hd))
        for r in (0, 1):
            for m in range(mems):
                maskb[j, r, m] = (side[:, r:r + 1] == float(m)).astype(F32).astype(BF16) * jnp.ones((tok, hd), BF16)
    atot[...] = jnp.exp(total)
    a_copy().start()
    for h in range(hl):
        pbuf[h, 0] = jnp.zeros((mems * hd, hd), BF16)

    def update(h):
        for t in (0, 1):
            own_token(t, h).wait()
            for there in peers:
                token_copy(t, h, there, there).wait_recv()
        state = jnp.zeros((mems * hd, hd), F32)
        for j in range(n):
            turned = kbuf[j, h].astype(F32).T
            keyed = jnp.concatenate(
                [(turned * kew[j, pl.ds(h * mems + m, 1), :]).astype(BF16) for m in range(mems)], axis=0)
            fresh = dot(keyed, vbuf[j, h])
            if j > 0:
                pbuf[h, j] = state.astype(BF16)
                state = jnp.concatenate(
                    [adec[j, pl.ds(h * mems + m, 1), :] * state[m * hd:(m + 1) * hd] for m in range(mems)],
                    axis=0) + fresh
            else:
                state = fresh
        for m in range(mems):
            u32[h, m] = state[m * hd:(m + 1) * hd]
            if m < direct:
                @pl.when(jnp.logical_or(even, jnp.logical_not(last)))
                def _():
                    ubf[h, m] = state[m * hd:(m + 1) * hd].astype(BF16)
                    u_copy(h, m).start()

    causal = row_at >= col_at

    def intra(h, j):
        query, value = qbuf[j, h], vbuf[j, h]
        score = dot(query, kbuf[j, h], ((1,), (1,)))
        query32 = query.astype(F32)
        col = cols[j, h]
        levels = [lrm[j, pl.ds(h * mems + m, 1), :] for m in range(mems)]
        left = []
        for r in (0, 1):
            ident = wide[j, r]
            level = levels[0]
            for m in range(1, mems):
                level = jnp.where(ident == float(m), levels[m], level)
            decay = jnp.exp(jnp.where(causal, col[:, r:r + 1] - level, -FAR))
            near_query = (query32 * col[:, 2 + r:3 + r]).astype(BF16)
            far_query = (query32 * col[:, 4 + r:5 + r]).astype(BF16)
            left.append(jnp.concatenate(
                [(decay * score).astype(BF16)] + [near_query * maskb[j, r, m] for m in range(mems)], axis=1))
            for m in range(mems):
                xbuf[h, j, r * tok:(r + 1) * tok, m * hd:(m + 1) * hd] = far_query * maskb[j, r, m]
        raw[h, j] = dot(jnp.concatenate(left, axis=0), jnp.concatenate([value, pbuf[h, j]], axis=0))

    def receive(h, m):
        @pl.when(first)
        def _():
            erecv[h, m] = jnp.zeros((hd, hd), BF16)

        @pl.when(jnp.logical_not(first))
        def _():
            e_copy(h, m).wait_recv()

    def relay_early(unit, carry):
        h = lax.div(unit, turned_later)
        m = direct + lax.rem(unit, turned_later)
        mine, other = atot[pl.ds(h * mems + m, 1), :], apart[pl.ds(h * mems + m, 1), :]
        receive(h, m)
        before = erecv[h, m].astype(F32)
        fresh = u32[h, m]

        @pl.when(jnp.logical_not(last))
        def _():
            esend[h, m] = (jnp.where(even, other, 1.0) * fresh + mine * other * before).astype(BF16)
            e_copy(h, m).start()

        @pl.when(jnp.logical_or(even, jnp.logical_not(first)))
        def _():
            ubf[h, m] = jnp.where(even, mine * before + fresh, before).astype(BF16)
            u_copy(h, m).start()

        return carry

    def relay_late(unit, carry):
        h = lax.div(unit, mems)
        m = lax.rem(unit, mems)
        mine, other = atot[pl.ds(unit, 1), :], apart[pl.ds(unit, 1), :]
        unsent = jnp.logical_and(even, jnp.where(m < direct, last, first))

        @pl.when(jnp.logical_not(unsent))
        def _():
            u_copy(h, m).wait_recv()

        @pl.when(m < direct)
        def _():
            receive(h, m)

            @pl.when(jnp.logical_not(last))
            def _():
                both = jnp.where(even, other, 1.0) * u32[h, m]
                both = both + jnp.where(even, 1.0, mine) * upart[h, m].astype(F32)
                esend[h, m] = (both + mine * other * erecv[h, m].astype(F32)).astype(BF16)
                e_copy(h, m).start()

            @pl.when(even)
            def _():
                sgrp[h, m] = erecv[h, m]

            @pl.when(jnp.logical_not(even))
            def _():
                sgrp[h, m] = (other * erecv[h, m].astype(F32) + upart[h, m].astype(F32)).astype(BF16)

        @pl.when(jnp.logical_and(m >= direct, unsent))
        def _():
            sgrp[h, m] = jnp.zeros((hd, hd), BF16)

        @pl.when(jnp.logical_and(m >= direct, jnp.logical_not(unsent)))
        def _():
            sgrp[h, m] = (jnp.where(even, 1.0, other) * erecv[h, m].astype(F32)
                          + upart[h, m].astype(F32)).astype(BF16)

        return carry

    def finish(h, j):
        gain = gainv[:, lanes(me * hl + h)]
        state = jnp.concatenate([sgrp[h, m] for m in range(mems)], axis=0)
        whole = raw[h, j] + dot(xbuf[h, j], state)
        mixed = jnp.zeros((tok, hd), F32)
        for r in (0, 1):
            part = whole[r * tok:(r + 1) * tok]
            scale = lax.rsqrt(jnp.mean(part * part, axis=-1, keepdims=True) + EPSILON)
            mixed = mixed + wide[j, 2 + r] * (part * scale).astype(BF16).astype(F32)
        outb[h, j] = (mixed * gain).astype(BF16)

    done = [0, 0]

    def catch_up(now, low, high):
        for stage, per, start in ((0, turned_later, EARLY_AT), (1, mems, LATE_AT)):
            since = now - start - rank * HOP + (64 + seqs) * HEAD_STEP
            whole = lax.div(since, HEAD_STEP)
            some = jnp.minimum(lax.div(since - whole * HEAD_STEP, PIECE_STEP) + 1, per)
            upto = jnp.clip((whole - 64 - seqs) * per + some, low * per, high * per)
            upto = jnp.maximum(upto, done[stage])
            lax.fori_loop(done[stage], upto, (relay_early, relay_late)[stage], 0)
            done[stage] = upto

    for h in range(hl):
        update(h)
        if h == 0:
            a_copy().wait_recv()
        now = KEYS_AT + h * HEAD_STEP + UPDATE_NS
        catch_up(now, 0, h + 1)
        own_token(2, h).wait()
        token_copy(2, h, near[0], near[0]).wait_recv()
        for j in [me] + near:
            intra(h, j)
            now += INTRA_NS
            catch_up(now, 0, h + 1)
        if h + 1 < hl:
            catch_up(KEYS_AT + (h + 1) * HEAD_STEP, 0, h + 1)

    def finish_all(h):
        for there in peers:
            finish(h, there)
            out_copy(h, there, me).start()
        finish(h, me)
        own_out(h).start()

    local_copy(1).wait()
    queries_at = KEYS_AT + (hl - 1) * HEAD_STEP + QUERY_STEP
    for h in range(hl):
        catch_up(queries_at + h * QUERY_STEP, max(h - 1, 0), hl)
        for i, there in enumerate(away):
            token_copy(2, h, there, there).wait_recv()
            intra(h, there)
            catch_up(queries_at + h * QUERY_STEP + (i + 1) * INTRA_NS, max(h - 1, 0), hl)
        if h == 1:
            catch_up(queries_at + h * QUERY_STEP + 2 * INTRA_NS, 1, hl)
            finish_all(0)
    for h in range(1 if hl > 1 else 0, hl):
        catch_up(queries_at + hl * QUERY_STEP + h * FINISH_NS, h + 1, hl)
        finish_all(h)

    for h in range(hl):
        own_out(h).wait()
    for there in peers:
        for t in range(3):
            aux_copy(t, there, me).wait_send()
        for h in range(hl):
            for t in range(3):
                token_copy(t, h, there, me).wait_send()
            out_copy(h, there, me).wait_send()
            out_copy(h, there, there).wait_recv()
    a_copy().wait_send()
    for h in range(hl):
        for m in range(mems):
            @pl.when(jnp.logical_or(even, jnp.logical_not(last if m < direct else first)))
            def _():
                u_copy(h, m).wait_send()

            @pl.when(jnp.logical_not(last))
            def _():
                e_copy(h, m).wait_send()


def body(n, seqs, queries, keys, values, gamma, rate, route_ids, route_weights, norm_gain):
    tok, feats = queries.shape
    heads = gamma.shape[1]
    mems = rate.shape[0]
    hd = feats // heads
    hl = heads // n
    pair = 2
    vm = pltpu.VMEM
    dma = pltpu.SemaphoreType.DMA
    rows = hl * mems
    buffers = [
        vm((n, hl, tok, hd), BF16), vm((n, hl, tok, hd), BF16), vm((n, hl, tok, hd), BF16),
        vm((n, heads, tok), BF16), vm((n, 2, tok), jnp.int32), vm((n, 2, tok), F32),
        vm(rate.shape, BF16), vm((1, feats), F32),
        vm((n, rows, tok), F32), vm((n, rows, tok), F32), vm((n, rows, tok), F32),
        vm((rows, tok), F32), vm((rows, tok), F32),
        vm((n, hl, tok, 8), F32), vm((n, 4, tok, hd), F32), vm((n, 2, mems, tok, hd), BF16),
        vm((hl, n, mems * hd, hd), BF16), vm((hl, n, 2 * tok, mems * hd), BF16),
        vm((hl, mems, hd, hd), F32), vm((hl, mems, hd, hd), BF16), vm((hl, mems, hd, hd), BF16),
        vm((hl, mems, hd, hd), BF16), vm((hl, mems, hd, hd), BF16), vm((hl, mems, hd, hd), BF16),
        vm((hl, n, 2 * tok, hd), F32),
        vm((hl, n, tok, hd), BF16),
    ]
    scratch = buffers + [
        dma((3, n)), dma((3, n)), dma((3, hl, n)), dma((3, hl, n)), dma((2,)), dma, dma,
        dma((hl, mems)), dma((hl, mems)), dma((hl, mems)), dma((hl, mems)), dma((hl, n)), dma((hl, n)), dma((hl,)),
    ]
    held = sum(math.prod(x.shape) * jnp.dtype(x.dtype).itemsize for x in buffers)
    grant = min(held + held // 8 + (12 << 20), 60 << 20)
    spec = pl.BlockSpec(memory_space=pl.ANY)
    return pl.pallas_call(
        functools.partial(kernel, n, seqs, hl, mems, pair),
        out_shape=jax.ShapeDtypeStruct((tok, feats), BF16),
        in_specs=[spec] * 8,
        out_specs=spec,
        scratch_shapes=scratch,
        compiler_params=pltpu.CompilerParams(
            collective_id=0, has_side_effects=True, vmem_limit_bytes=grant),
    )(*[pltpu.with_memory_space_constraint(x, pltpu.HBM) for x in (queries, keys, values, gamma.T, rate, route_ids.T, route_weights.T, norm_gain.reshape(1, feats))])


def solution(mesh):
    rows = P(("seq", "mem"), None)
    in_specs = (rows, rows, rows, rows, P(), rows, rows, P())
    run = functools.partial(body, mesh.shape["mem"], mesh.shape["seq"])
    return jax.shard_map(run, mesh=mesh, in_specs=in_specs, out_specs=rows, check_vma=False)
```
